32 devices in a mesh: row: 2 (over core), col: 4 (over y, x), depth: 4 (over z).
Axes of the slice: x: 2, y: 2, z: 4, core: 2. Of those that a mesh axis runs over, the one named last changes fastest.
Arguments:
- a_tile: float32 [2048, 2048], P('row', 'col'), as said below
- panels: float32 [2048, 4096], P('row', 'depth'), as said below
Outputs:
- trailing: float32 [2048, 2048], P(('row', 'depth'), 'col')
- new_panel: float32 [2048, 512], P(('row', 'col'))
- diag_norm: float32 [1], replicated
Inputs may be any that keep to these rules, and one draw needn't show every extreme that they name: symmetric; a_tile - panels panels^T is positive definite with a large positive diagonal. `panels`: real-valued entries of full rank.
All inputs are finite; a program needn't handle non-finite values.
Results may differ from the reference program's by a relative error of at most 0.00015.
Values sent between devices are 32-bit elements; how exact they have to be, the bound alone decides.
A program may use at most 64 MiB of HBM per device.

```python
import jax
import jax.numpy as jnp
from jax import lax

PB = 512
M = 2048
KTOT = 4096


def panel_matrix(key):
    key_panel = jax.random.fold_in(key, 21)
    deviation = jnp.sqrt(1.5 / jnp.sqrt(jnp.float32(M) * jnp.float32(KTOT)))
    base = jnp.clip(jax.random.normal(key_panel, (M, KTOT), jnp.float32), -6.0, 6.0)
    return (base * deviation).astype(jnp.float32)


def draw_panels(key, part):
    return panel_matrix(key)


def draw_a_tile(key, part):
    key_noise = jax.random.fold_in(key, 11)
    key_diag = jax.random.fold_in(key, 12)
    noise = jax.random.normal(key_noise, (M, M), jnp.float32)
    spread = jax.random.uniform(key_diag, (M,), jnp.float32, 1.0, 1.5)
    noise = noise * (0.5 / jnp.sqrt(jnp.float32(M)))
    symmetric = (noise + noise.T) * 0.7071
    rising = jnp.power(3.0, jnp.arange(M, dtype=jnp.float32) / M)
    diagonal = 4.0 * rising * spread
    panel_full = panel_matrix(key)
    product = jnp.dot(panel_full, panel_full.T, precision=lax.Precision.HIGHEST, preferred_element_type=jnp.float32)
    product = (product + product.T) * 0.5
    return (symmetric + jnp.diag(diagonal) + product).astype(jnp.float32)


def setup_inputs(seed: int = 0) -> dict:
    splits = jax.random.split(jax.random.key(seed), 3)
    a_tile = draw_a_tile(jax.random.fold_in(splits[2], 71), 0)
    panels = draw_panels(jax.random.fold_in(splits[2], 71), 0)
    return dict(a_tile=a_tile, panels=panels)


def reference(a_tile, panels):
    product = jnp.dot(panels.astype(jnp.float32), panels.T.astype(jnp.float32), precision=lax.Precision.HIGHEST, preferred_element_type=jnp.float32)
    trailing = a_tile - product
    factor = jnp.linalg.cholesky(trailing[:PB, :PB])
    new_panel = jax.scipy.linalg.solve_triangular(factor, trailing[:, :PB].T, lower=True).T
    diagonal = jnp.diagonal(trailing)
    diag_norm = jnp.sqrt(jnp.sum(diagonal * diagonal) / M).reshape(1)
    return (trailing, new_panel, diag_norm)
```

```python
import functools

import jax
import jax.numpy as jnp
from jax import lax
from jax.experimental import pallas as pl
from jax.experimental.pallas import tpu as pltpu
from jax.sharding import PartitionSpec as P

PB = 512
BLOCK = 128
NB = 32
CHUNK = 128
TILE = 256
HIGHEST = lax.Precision.HIGHEST
MESH = pl.DeviceIdType.MESH
F32 = jnp.float32
BF16 = jnp.bfloat16


def split(value):
    high = value.astype(BF16)
    return high, (value - high.astype(F32)).astype(BF16)


def dot_t(left, right):
    return lax.dot_general(left, right, (((1,), (1,)), ((), ())), preferred_element_type=F32)


def product(left_hi, left_lo, right_hi, right_lo):
    return dot_t(left_hi, right_hi) + (dot_t(left_hi, right_lo) + dot_t(left_lo, right_hi))


def gather_update(sizes, a_ref, p_ref, out_ref, c_ref, d_ref, n_ref, *scratch):
    nr, nc, nd = sizes
    (own_hi, own_lo, oth_hi, oth_lo, p0, pc, part, up, down, cpart, crecv, arow, nbuf, psum,
     pair_send, pair_recv, a_send, a_recv, rs_send, rs_recv, ag_send, ag_recv, d_send, d_recv,
     f_send, f_recv, up_send, up_recv, down_send, down_recv, n_send, n_recv) = scratch
    tile_rows, tile_cols = a_ref.shape
    share = tile_rows // nd
    crows = tile_rows // nc
    piece = crows // nd
    heads = PB // crows
    r, c, z = lax.axis_index("row"), lax.axis_index("col"), lax.axis_index("depth")
    chunks = tile_cols // CHUNK

    def at(row, col, depth):
        return (row, col, depth)

    def remote(src, dst, send, recv, device):
        return pltpu.make_async_remote_copy(
            src_ref=src, dst_ref=dst, send_sem=send, recv_sem=recv, device_id=device, device_id_type=MESH)

    def rows(start, size):
        return pl.ds(pl.multiple_of(start, size), size)

    barrier = pltpu.get_barrier_semaphore()
    for k in range(1, nd):
        pl.semaphore_signal(barrier, inc=1, device_id=at(r, c, lax.rem(z + k, nd)), device_id_type=MESH)
    for m in range(1, nc):
        pl.semaphore_signal(barrier, inc=1, device_id=at(r, lax.rem(c + m, nc), z), device_id_type=MESH)
    pl.semaphore_signal(barrier, inc=1, device_id=at(1 - r, c, z), device_id_type=MESH)

    @pl.loop(0, tile_rows // TILE)
    def _(t):
        hi, lo = split(p_ref[rows(t * TILE, TILE), :])
        own_hi[rows(t * TILE, TILE), :] = hi
        own_lo[rows(t * TILE, TILE), :] = lo

    pl.semaphore_wait(barrier, nd - 1 + nc - 1 + 1)

    partner = at(1 - r, c, z)
    first = c * tile_cols
    owner = first // tile_rows
    offset = lax.rem(first, tile_rows)
    head_copy = remote(p_ref.at[pl.ds(0, PB), :], p0, pair_send.at[0], pair_recv.at[0], partner)
    col_copy = remote(p_ref.at[rows(offset, tile_cols), :], pc, pair_send.at[1], pair_recv.at[1], partner)

    def a_copy(m):
        to = lax.rem(c + m, nc)
        return remote(a_ref.at[rows(to * crows + z * piece, piece), pl.ds(0, PB)], arow,
                      a_send.at[m], a_recv, at(r, to, z))

    @pl.when(r == 0)
    def _():
        head_copy.start()

    @pl.when(c == 0)
    def _():
        for m in range(1, nc):
            a_copy(m).start()

    @pl.when(r == owner)
    def _():
        col_copy.start()

    @pl.when(r == 0)
    def _():
        oth_hi[...] = own_hi[pl.ds(0, PB), :]
        oth_lo[...] = own_lo[pl.ds(0, PB), :]

    @pl.when(r != 0)
    def _():
        head_copy.wait_recv()
        hi, lo = split(p0[...])
        oth_hi[...] = hi
        oth_lo[...] = lo

    mine = rows(c * crows, crows)
    cpart[...] = product(own_hi[mine, :], own_lo[mine, :], oth_hi[...], oth_lo[...])

    def rs_copy(k):
        to = lax.rem(z + k, nd)
        return remote(cpart.at[rows(to * piece, piece), :], crecv.at[k], rs_send.at[k], rs_recv.at[k], at(r, c, to))

    for k in range(1, nd):
        rs_copy(k).start()

    @pl.when(r == owner)
    def _():
        oth_hi[...] = own_hi[rows(offset, tile_cols), :]
        oth_lo[...] = own_lo[rows(offset, tile_cols), :]

    @pl.when(r != owner)
    def _():
        col_copy.wait_recv()
        hi, lo = split(pc[...])
        oth_hi[...] = hi
        oth_lo[...] = lo

    @pl.loop(0, tile_rows // TILE)
    def _(t):
        at_rows = rows(t * TILE, TILE)
        part[at_rows, :] = product(own_hi[at_rows, :], own_lo[at_rows, :], oth_hi[...], oth_lo[...])

    @pl.when(c == 0)
    def _():
        arow[...] = a_ref[rows(z * piece, piece), pl.ds(0, PB)]

    @pl.when(c != 0)
    def _():
        a_copy(1).wait_recv()

    total = cpart[rows(z * piece, piece), :]
    for k in range(1, nd):
        rs_copy(k).wait_recv()
        total = total + crecv[k]
    c_ref[rows(z * piece, piece), :] = arow[...] - total

    def ag_copy(k):
        here = rows(z * piece, piece)
        return remote(c_ref.at[here, :], c_ref.at[here, :], ag_send.at[k], ag_recv.at[k],
                      at(r, c, lax.rem(z + k, nd)))

    def ag_from(k):
        there = rows(lax.rem(z - k + nd, nd) * piece, piece)
        return remote(c_ref.at[there, :], c_ref.at[there, :], ag_send.at[k], ag_recv.at[k], at(r, c, lax.rem(z + k, nd)))

    def d_rows(head, k):
        return rows(head * crows + lax.rem(z - k + nd, nd) * piece, piece)

    def d_copy(k, m):
        return remote(c_ref.at[rows(lax.rem(z - k + nd, nd) * piece, piece), :], d_ref.at[d_rows(c, k), :],
                      d_send.at[k, m], d_recv.at[lax.rem(c, heads), k], at(r, lax.rem(c + m, nc), z))

    def f_copy(head, k):
        return remote(d_ref.at[d_rows(head, k), :], d_ref.at[d_rows(head, k), :],
                      f_send.at[head, k], f_recv.at[head, k], partner)

    def d_from(head, k):
        return remote(d_ref.at[d_rows(head, k), :], d_ref.at[d_rows(head, k), :],
                      d_send.at[k, 0], d_recv.at[head, k], partner)

    for k in range(1, nd):
        ag_copy(k).start()
    source = jnp.logical_and(r == 0, c < heads)
    for k in range(nd):
        if k:
            ag_from(k).wait_recv()

        @pl.when(source)
        def _():
            for m in range(1, nc):
                d_copy(k, m).start()

    @pl.when(r == 0)
    def _():
        for k in range(nd):
            for head in range(heads):
                @pl.when(c == head)
                def _():
                    d_ref[d_rows(head, k), :] = c_ref[rows(lax.rem(z - k + nd, nd) * piece, piece), :]

                @pl.when(c != head)
                def _():
                    d_from(head, k).wait_recv()

                f_copy(head, k).start()

    def up_copy(b, ch):
        lanes = rows(ch * CHUNK, CHUNK)
        return remote(part.at[rows(b * share, share), lanes], up.at[rows(b * share, share), lanes],
                      up_send.at[b, ch], up_recv.at[b, ch], at(r, c, lax.rem(z + 1, nd)))

    def down_copy(b, ch):
        lanes = rows(ch * CHUNK, CHUNK)
        return remote(down_src.at[rows(b * share, share), lanes], down.at[rows(b * share, share), lanes],
                      down_send.at[b, ch], down_recv.at[b, ch], at(r, c, lax.rem(z + nd - 1, nd)))

    down_src = part

    def tick(i):
        u = i - z
        @pl.when(jnp.logical_and(u >= 0, u < (nd - z) * chunks))
        def _():
            b = nd - 1 - u // chunks
            ch = lax.rem(u, chunks)
            here = (rows(b * share, share), rows(ch * CHUNK, CHUNK))

            @pl.when(z > 0)
            def _():
                up_copy(b, ch).wait_recv()
                part[here] = part[here] + up[here]

            @pl.when(b > z)
            def _():
                up_copy(b, ch).start()

        v = i - (nd - 1 - z)
        @pl.when(jnp.logical_and(v >= 0, v < (z + 1) * chunks))
        def _():
            b = v // chunks
            ch = lax.rem(v, chunks)
            here = (rows(b * share, share), rows(ch * CHUNK, CHUNK))

            @pl.when(z < nd - 1)
            def _():
                down_copy(b, ch).wait_recv()
                part[here] = part[here] + down[here]

            @pl.when(b < z)
            def _():
                down_copy(b, ch).start()

    pl.loop(0, nd * chunks + nd - 1)(tick)

    trailing = a_ref[rows(z * share, share), :] - part[rows(z * share, share), :]
    out_ref[...] = trailing
    grow = r * tile_rows + z * share + lax.broadcasted_iota(jnp.int32, trailing.shape, 0)
    gcol = first + lax.broadcasted_iota(jnp.int32, trailing.shape, 1)
    squares = jnp.where(grow == gcol, trailing * trailing, 0.0)
    acc = squares.reshape(share // 8, 8, tile_cols).sum(0)
    acc = acc.reshape(8, chunks, CHUNK).sum(1) if chunks == 1 else sum(
        acc[:, i * CHUNK:(i + 1) * CHUNK] for i in range(chunks))
    psum[0] = acc

    stages = ((nd, lambda k: at(r, c, lax.rem(z + k, nd))), (nc, lambda k: at(r, lax.rem(c + k, nc), z)),
              (nr, lambda k: partner))
    base = 0
    for stage, (count, peer) in enumerate(stages):
        def n_copy(k):
            return remote(psum.at[stage], nbuf.at[base + k], n_send.at[base + k], n_recv.at[base + k], peer(k))
        for k in range(1, count):
            n_copy(k).start()
        for k in range(1, count):
            n_copy(k).wait_recv()
            acc = acc + nbuf[base + k]
        psum[stage + 1] = acc
        for k in range(1, count):
            n_copy(k).wait_send()
        base += count
    n_ref[...] = jnp.sqrt(jnp.sum(acc, keepdims=True) / (tile_cols * nc))

    @pl.when(r != 0)
    def _():
        for k in range(nd):
            for head in range(heads):
                f_copy(head, k).wait_recv()

    @pl.when(r == 0)
    def _():
        head_copy.wait_send()
        for k in range(nd):
            for head in range(heads):
                f_copy(head, k).wait_send()

    @pl.when(r == owner)
    def _():
        col_copy.wait_send()

    @pl.when(c == 0)
    def _():
        for m in range(1, nc):
            a_copy(m).wait_send()

    @pl.when(source)
    def _():
        for k in range(nd):
            for m in range(1, nc):
                d_copy(k, m).wait_send()

    for k in range(1, nd):
        rs_copy(k).wait_send()
        ag_copy(k).wait_send()

    @pl.loop(0, nd)
    def _(b):
        for ch in range(chunks):
            @pl.when(b > z)
            def _():
                up_copy(b, ch).wait_send()

            @pl.when(b < z)
            def _():
                down_copy(b, ch).wait_send()


def mm(a, b, dims):
    return lax.dot_general(a, b, (dims, ((), ())), precision=HIGHEST, preferred_element_type=F32)


def factor_block(block, work):
    work[:, :BLOCK] = block
    diag = lax.broadcasted_iota(jnp.int32, (BLOCK, BLOCK), 0) == lax.broadcasted_iota(jnp.int32, (BLOCK, BLOCK), 1)
    work[:, BLOCK:] = jnp.where(diag, 1.0, 0.0)
    sub = lax.broadcasted_iota(jnp.int32, (NB, BLOCK), 0)
    for j in range(0, BLOCK, NB):
        left = work[j:j + NB, :BLOCK]
        right = work[j:j + NB, BLOCK:]
        lanes = [jnp.broadcast_to(left[:, j + k:j + k + 1], (NB, BLOCK)) for k in range(NB)]
        for k in range(NB):
            inv = lax.rsqrt(lanes[k][k:k + 1])
            col = lanes[k] * inv
            for i in range(k + 1, NB):
                lanes[i] = lanes[i] - col * col[i:i + 1]
            row_l = left[k:k + 1] * inv
            row_r = right[k:k + 1] * inv
            below = jnp.where(sub > k, col, 0.0)
            left = jnp.where(sub == k, row_l, left - below * row_l)
            right = jnp.where(sub == k, row_r, right - below * row_r)
        work[j:j + NB, :BLOCK] = left
        work[j:j + NB, BLOCK:] = right
        if j + NB < BLOCK:
            both = jnp.concatenate([left, right], axis=1)
            work[j + NB:, :] = work[j + NB:, :] - mm(left[:, j + NB:], both, ((0,), (0,)))
    return work[:, BLOCK:]


def chol_solve(d_ref, c_ref, out_ref, a, c, work):
    size = d_ref.shape[0]
    a[...] = d_ref[...]
    c[...] = c_ref[...]
    for s in range(0, size, BLOCK):
        e = s + BLOCK
        inv = factor_block(a[s:e, s:e], work)
        x = mm(c[:, s:e], inv, ((1,), (1,)))
        out_ref[:, s:e] = x
        if e < size:
            u = mm(inv, a[s:e, e:], ((1,), (0,)))
            a[e:, e:] = a[e:, e:] - mm(u, u, ((0,), (0,)))
            c[:, e:] = c[:, e:] - mm(x, u, ((1,), (0,)))


def local(sizes, a_tile, panels):
    nr, nc, nd = sizes
    tile_rows, tile_cols = a_tile.shape
    k_size = panels.shape[1]
    share, crows = tile_rows // nd, tile_rows // nc
    piece, heads, chunks = crows // nd, PB // crows, tile_cols // CHUNK
    vmem = pl.BlockSpec(memory_space=pltpu.VMEM)
    shape = lambda *s: jax.ShapeDtypeStruct(s, F32)
    dma = lambda *s: pltpu.SemaphoreType.DMA(s)
    wide = max(PB, tile_cols)
    trailing, rows_c, diag, norm = pl.pallas_call(
        functools.partial(gather_update, sizes),
        out_shape=(shape(share, tile_cols), shape(crows, PB), shape(PB, PB), shape(1, 1)),
        in_specs=[vmem] * 2,
        out_specs=(vmem,) * 4,
        scratch_shapes=[
            pltpu.VMEM((tile_rows, k_size), BF16), pltpu.VMEM((tile_rows, k_size), BF16),
            pltpu.VMEM((wide, k_size), BF16), pltpu.VMEM((wide, k_size), BF16),
            pltpu.VMEM((PB, k_size), F32), pltpu.VMEM((tile_cols, k_size), F32),
            pltpu.VMEM((tile_rows, tile_cols), F32), pltpu.VMEM((tile_rows, tile_cols), F32),
            pltpu.VMEM((tile_rows, tile_cols), F32), pltpu.VMEM((crows, PB), F32),
            pltpu.VMEM((nd, piece, PB), F32), pltpu.VMEM((piece, PB), F32),
            pltpu.VMEM((nr + nc + nd, 8, CHUNK), F32), pltpu.VMEM((4, 8, CHUNK), F32),
            dma(2), dma(2), dma(nc), pltpu.SemaphoreType.DMA, dma(nd), dma(nd), dma(nd), dma(nd),
            dma(nd, nc), dma(heads, nd), dma(heads, nd), dma(heads, nd),
            dma(nd, chunks), dma(nd, chunks), dma(nd, chunks), dma(nd, chunks),
            dma(nr + nc + nd), dma(nr + nc + nd),
        ],
        compiler_params=pltpu.CompilerParams(collective_id=0, has_side_effects=True, vmem_limit_bytes=60 << 20),
        name="gather_update",
    )(a_tile, panels)
    new_panel = pl.pallas_call(
        chol_solve,
        out_shape=shape(crows, PB),
        in_specs=[vmem] * 2,
        out_specs=vmem,
        scratch_shapes=[pltpu.VMEM((PB, PB), F32), pltpu.VMEM((crows, PB), F32), pltpu.VMEM((BLOCK, 2 * BLOCK), F32)],
        name="chol_solve",
    )(diag, rows_c)
    return (trailing, new_panel, norm.reshape(1))


def solution(mesh):
    sizes = tuple(mesh.shape[axis] for axis in ("row", "col", "depth"))
    return jax.shard_map(
        functools.partial(local, sizes),
        mesh=mesh,
        in_specs=(P("row", "col"), P("row", "depth")),
        out_specs=(P(("row", "depth"), "col"), P(("row", "col"), None), P()),
        check_vma=False,
    )
```

```python
import functools

import jax
import jax.numpy as jnp
from jax import lax
from jax.experimental import pallas as pl
from jax.experimental.pallas import tpu as pltpu
from jax.sharding import PartitionSpec as P

PB = 512
BLOCK = 128
NB = 32
CHUNK = 128
EARLY = 3
TILE = 256
HIGHEST = lax.Precision.HIGHEST
MESH = pl.DeviceIdType.MESH
F32 = jnp.float32
BF16 = jnp.bfloat16


def split(value):
    high = value.astype(BF16)
    return high, (value - high.astype(F32)).astype(BF16)


def dot_t(left, right):
    return lax.dot_general(left, right, (((1,), (1,)), ((), ())), preferred_element_type=F32)


def product(left_hi, left_lo, right_hi, right_lo):
    return dot_t(left_hi, right_hi) + (dot_t(left_hi, right_lo) + dot_t(left_lo, right_hi))


def mm(a, b, dims):
    return lax.dot_general(a, b, (dims, ((), ())), precision=HIGHEST, preferred_element_type=F32)


def factor_block(work, block, advance):
    work[:, :BLOCK] = block
    diag = lax.broadcasted_iota(jnp.int32, (BLOCK, BLOCK), 0) == lax.broadcasted_iota(jnp.int32, (BLOCK, BLOCK), 1)
    work[:, BLOCK:] = jnp.where(diag, 1.0, 0.0)
    sub = lax.broadcasted_iota(jnp.int32, (NB, BLOCK), 0)
    for j in range(0, BLOCK, NB):
        left = work[j:j + NB, :BLOCK]
        right = work[j:j + NB, BLOCK:]
        advance()
        lanes = [jnp.broadcast_to(left[:, j + k:j + k + 1], (NB, BLOCK)) for k in range(NB)]
        for k in range(NB):
            inv = lax.rsqrt(lanes[k][k:k + 1])
            col = lanes[k] * inv
            for i in range(k + 1, NB):
                lanes[i] = lanes[i] - col * col[i:i + 1]
            row_l = left[k:k + 1] * inv
            row_r = right[k:k + 1] * inv
            below = jnp.where(sub > k, col, 0.0)
            left = jnp.where(sub == k, row_l, left - below * row_l)
            right = jnp.where(sub == k, row_r, right - below * row_r)
        work[j:j + NB, :BLOCK] = left
        work[j:j + NB, BLOCK:] = right
        if j + NB < BLOCK:
            both = jnp.concatenate([left, right], axis=1)
            work[j + NB:, :] = work[j + NB:, :] - mm(left[:, j + NB:], both, ((0,), (0,)))
    return work[:, BLOCK:]


def gather_update(sizes, split_d, a_ref, p_ref, out_ref, x_ref, n_ref, *scratch):
    nr, nc, nd = sizes
    (own_hi, own_lo, oth_hi, oth_lo, p0, pc, part, up, down, cpart, crecv, arow, nbuf, psum,
     pair_send, pair_recv, a_send, a_recv, rs_send, rs_recv, ag_send, ag_recv, d_send, d_recv,
     f_send, f_recv, up_send, up_recv, down_send, down_recv, n_send, n_recv,
     c_ref, d_ref, work, invs, fact, rest, dpart, drecv, adiag, ds_send, ds_recv, da_send, da_recv, ad_send, ad_recv) = scratch
    tile_rows, tile_cols = a_ref.shape
    share = tile_rows // nd
    crows = tile_rows // nc
    piece = crows // nd
    slab = PB // nc
    d_high, d_wide = split_d
    r, c, z = lax.axis_index("row"), lax.axis_index("col"), lax.axis_index("depth")
    chunks = tile_cols // CHUNK

    def at(row, col, depth):
        return (row, col, depth)

    def remote(src, dst, send, recv, device):
        return pltpu.make_async_remote_copy(
            src_ref=src, dst_ref=dst, send_sem=send, recv_sem=recv, device_id=device, device_id_type=MESH)

    def rows(start, size):
        return pl.ds(pl.multiple_of(start, size), size)

    barrier = pltpu.get_barrier_semaphore()
    for k in range(1, nd):
        pl.semaphore_signal(barrier, inc=1, device_id=at(r, c, lax.rem(z + k, nd)), device_id_type=MESH)
    for m in range(1, nc):
        pl.semaphore_signal(barrier, inc=1, device_id=at(r, lax.rem(c + m, nc), z), device_id_type=MESH)
    pl.semaphore_signal(barrier, inc=1, device_id=at(1 - r, c, z), device_id_type=MESH)

    def split_own(t):
        hi, lo = split(p_ref[rows(t * TILE, TILE), :])
        own_hi[rows(t * TILE, TILE), :] = hi
        own_lo[rows(t * TILE, TILE), :] = lo

    pl.loop(0, PB // TILE)(split_own)
    pl.semaphore_wait(barrier, nd - 1 + nc - 1 + 1)

    partner = at(1 - r, c, z)
    first = c * tile_cols
    owner = first // tile_rows
    offset = lax.rem(first, tile_rows)
    head_copy = remote(p_ref.at[pl.ds(0, PB), :], p0, pair_send.at[0], pair_recv.at[0], partner)
    col_copy = remote(p_ref.at[rows(offset, tile_cols), :], pc, pair_send.at[1], pair_recv.at[1], partner)

    def a_copy(m):
        to = lax.rem(c + m, nc)
        return remote(a_ref.at[rows(to * crows + z * piece, piece), pl.ds(0, PB)], arow,
                      a_send.at[m], a_recv, at(r, to, z))

    def patch(depth):
        return (rows(depth // (PB // d_wide) * d_high, d_high),
                rows(lax.rem(depth, PB // d_wide) * d_wide, d_wide))

    def in_slab(col, depth):
        high, wide = patch(depth)
        return (rows(col * slab + depth // (PB // d_wide) * d_high, d_high), wide)

    def ad_copy(m):
        to = lax.rem(c + m, nc)
        return remote(a_ref.at[in_slab(to, z)], adiag, ad_send.at[m], ad_recv, at(r, to, z))

    def ds_copy(k):
        to = lax.rem(z + k, nd)
        return remote(dpart.at[patch(to)], drecv.at[k], ds_send.at[k], ds_recv.at[k], at(r, c, to))

    def da_copy(k):
        here = d_ref.at[in_slab(c, z)]
        return remote(here, here, da_send.at[k], da_recv.at[k], at(r, c, lax.rem(z + k, nd)))

    def da_from(k):
        there = d_ref.at[in_slab(c, lax.rem(z - k + nd, nd))]
        return remote(there, there, da_send.at[k], da_recv.at[k], at(r, c, lax.rem(z + k, nd)))

    @pl.when(r == 0)
    def _():
        head_copy.start()

        @pl.when(c == 0)
        def _():
            for m in range(1, nc):
                ad_copy(m).start()

    @pl.when(c == 0)
    def _():
        for m in range(1, nc):
            a_copy(m).start()

    @pl.when(r == owner)
    def _():
        col_copy.start()

    @pl.when(r == 0)
    def _():
        oth_hi[...] = own_hi[pl.ds(0, PB), :]
        oth_lo[...] = own_lo[pl.ds(0, PB), :]
        band = rows(c * slab, slab)
        dpart[...] = product(own_hi[band, :], own_lo[band, :], oth_hi[...], oth_lo[...])
        for k in range(1, nd):
            ds_copy(k).start()

    pl.loop(PB // TILE, tile_rows // TILE)(split_own)

    @pl.when(r != 0)
    def _():
        head_copy.wait_recv()
        hi, lo = split(p0[...])
        oth_hi[...] = hi
        oth_lo[...] = lo

    mine = rows(c * crows, crows)
    cpart[...] = product(own_hi[mine, :], own_lo[mine, :], oth_hi[...], oth_lo[...])

    def rs_copy(k):
        to = lax.rem(z + k, nd)
        return remote(cpart.at[rows(to * piece, piece), :], crecv.at[k], rs_send.at[k], rs_recv.at[k], at(r, c, to))

    for k in range(1, nd):
        rs_copy(k).start()

    @pl.when(r == 0)
    def _():
        @pl.when(c == 0)
        def _():
            adiag[...] = a_ref[in_slab(0, z)]

        @pl.when(c != 0)
        def _():
            ad_copy(1).wait_recv()

        dsum = dpart[patch(z)]
        for k in range(1, nd):
            ds_copy(k).wait_recv()
            dsum = dsum + drecv[k]
        d_ref[in_slab(c, z)] = adiag[...] - dsum
        for k in range(1, nd):
            da_copy(k).start()

    @pl.when(r == owner)
    def _():
        oth_hi[...] = own_hi[rows(offset, tile_cols), :]
        oth_lo[...] = own_lo[rows(offset, tile_cols), :]

    @pl.when(r != owner)
    def _():
        col_copy.wait_recv()
        hi, lo = split(pc[...])
        oth_hi[...] = hi
        oth_lo[...] = lo

    @pl.loop(0, tile_rows // TILE)
    def _(t):
        at_rows = rows(t * TILE, TILE)
        part[at_rows, :] = product(own_hi[at_rows, :], own_lo[at_rows, :], oth_hi[...], oth_lo[...])

    def d_piece(col, k):
        return d_ref.at[in_slab(col, lax.rem(z - k + nd, nd))]

    def d_copy(k, m):
        return remote(d_piece(c, k), d_piece(c, k), d_send.at[k, m], d_recv.at[k, m], at(r, lax.rem(c + m, nc), z))

    def d_from(k, m):
        there = d_piece(lax.rem(c - m + nc, nc), k)
        return remote(there, there, d_send.at[k, m], d_recv.at[k, m], at(r, lax.rem(c + m, nc), z))

    def f_copy(k, m):
        there = d_piece(lax.rem(c - m + nc, nc), k)
        return remote(there, there, f_send.at[k, m], f_recv.at[k, m], partner)

    @pl.when(r == 0)
    def _():
        for k in range(nd):
            if k:
                da_from(k).wait_recv()
            for m in range(1, nc):
                d_copy(k, m).start()
            f_copy(k, 0).start()

    @pl.when(c == 0)
    def _():
        arow[...] = a_ref[rows(z * piece, piece), pl.ds(0, PB)]

    @pl.when(c != 0)
    def _():
        a_copy(1).wait_recv()

    total = cpart[rows(z * piece, piece), :]
    for k in range(1, nd):
        rs_copy(k).wait_recv()
        total = total + crecv[k]
    c_ref[rows(z * piece, piece), :] = arow[...] - total

    def ag_copy(k):
        here = rows(z * piece, piece)
        return remote(c_ref.at[here, :], c_ref.at[here, :], ag_send.at[k], ag_recv.at[k],
                      at(r, c, lax.rem(z + k, nd)))

    def ag_from(k):
        there = rows(lax.rem(z - k + nd, nd) * piece, piece)
        return remote(c_ref.at[there, :], c_ref.at[there, :], ag_send.at[k], ag_recv.at[k], at(r, c, lax.rem(z + k, nd)))

    for k in range(1, nd):
        ag_copy(k).start()

    def up_copy(b, ch):
        lanes = rows(ch * CHUNK, CHUNK)
        return remote(part.at[rows(b * share, share), lanes], up.at[rows(b * share, share), lanes],
                      up_send.at[b, ch], up_recv.at[b, ch], at(r, c, lax.rem(z + 1, nd)))

    def down_copy(b, ch):
        lanes = rows(ch * CHUNK, CHUNK)
        return remote(part.at[rows(b * share, share), lanes], down.at[rows(b * share, share), lanes],
                      down_send.at[b, ch], down_recv.at[b, ch], at(r, c, lax.rem(z + nd - 1, nd)))

    def tick(i):
        u = i - z
        @pl.when(jnp.logical_and(u >= 0, u < (nd - z) * chunks))
        def _():
            b = nd - 1 - u // chunks
            ch = lax.rem(u, chunks)
            here = (rows(b * share, share), rows(ch * CHUNK, CHUNK))

            @pl.when(z > 0)
            def _():
                up_copy(b, ch).wait_recv()
                part[here] = part[here] + up[here]

            @pl.when(b > z)
            def _():
                up_copy(b, ch).start()

        v = i - (nd - 1 - z)
        @pl.when(jnp.logical_and(v >= 0, v < (z + 1) * chunks))
        def _():
            b = v // chunks
            ch = lax.rem(v, chunks)
            here = (rows(b * share, share), rows(ch * CHUNK, CHUNK))

            @pl.when(z < nd - 1)
            def _():
                down_copy(b, ch).wait_recv()
                part[here] = part[here] + down[here]

            @pl.when(b < z)
            def _():
                down_copy(b, ch).start()

    ticks = nd * chunks + nd - 1
    slots = PB // NB + EARLY
    done = []

    def advance(last=False):
        first_tick = len(done) * ticks // slots
        done.append(None)
        pl.loop(first_tick, ticks if last else min(ticks, len(done) * ticks // slots))(tick)

    for _ in range(EARLY):
        advance()

    @pl.when(r == 0)
    def _():
        for k in range(nd):
            for m in range(1, nc):
                d_from(k, m).wait_recv()
                f_copy(k, m).start()

    @pl.when(r != 0)
    def _():
        for k in range(nd):
            for m in range(nc):
                f_copy(k, m).wait_recv()

    for s in range(0, PB, BLOCK):
        e = s + BLOCK
        inv = factor_block(work, (fact if s else d_ref)[s:e, s:e], advance)
        invs[s // BLOCK] = inv
        if e < PB:
            u = mm(inv, (fact if s else d_ref)[s:e, e:], ((1,), (0,)))
            fact[s:e, e:] = u
            fact[e:, e:] = (fact if s else d_ref)[e:, e:] - mm(u, u, ((0,), (0,)))

    for k in range(1, nd):
        ag_from(k).wait_recv()
    rest[...] = c_ref[...]
    for s in range(0, PB, BLOCK):
        e = s + BLOCK
        x = mm(rest[:, s:e], invs[s // BLOCK], ((1,), (1,)))
        x_ref[:, s:e] = x
        if e < PB:
            rest[:, e:] = rest[:, e:] - mm(x, fact[s:e, e:], ((1,), (0,)))

    trailing = a_ref[rows(z * share, share), :] - part[rows(z * share, share), :]
    out_ref[...] = trailing
    grow = r * tile_rows + z * share + lax.broadcasted_iota(jnp.int32, trailing.shape, 0)
    gcol = first + lax.broadcasted_iota(jnp.int32, trailing.shape, 1)
    squares = jnp.where(grow == gcol, trailing * trailing, 0.0)
    acc = squares.reshape(share // 8, 8, tile_cols).sum(0)
    acc = acc.reshape(8, chunks, CHUNK).sum(1) if chunks == 1 else sum(
        acc[:, i * CHUNK:(i + 1) * CHUNK] for i in range(chunks))
    psum[0] = acc

    stages = ((nd, lambda k: at(r, c, lax.rem(z + k, nd))), (nc, lambda k: at(r, lax.rem(c + k, nc), z)),
              (nr, lambda k: partner))
    base = 0
    for stage, (count, peer) in enumerate(stages):
        def n_copy(k):
            return remote(psum.at[stage], nbuf.at[base + k], n_send.at[base + k], n_recv.at[base + k], peer(k))
        for k in range(1, count):
            n_copy(k).start()
        for k in range(1, count):
            n_copy(k).wait_recv()
            acc = acc + nbuf[base + k]
        psum[stage + 1] = acc
        for k in range(1, count):
            n_copy(k).wait_send()
        base += count
    n_ref[...] = jnp.sqrt(jnp.sum(acc, keepdims=True) / (tile_cols * nc))

    @pl.when(r == 0)
    def _():
        head_copy.wait_send()

        @pl.when(c == 0)
        def _():
            for m in range(1, nc):
                ad_copy(m).wait_send()

        for k in range(nd):
            for m in range(nc):
                f_copy(k, m).wait_send()
                if m:
                    d_copy(k, m).wait_send()
            if k:
                ds_copy(k).wait_send()
                da_copy(k).wait_send()

    @pl.when(r == owner)
    def _():
        col_copy.wait_send()

    @pl.when(c == 0)
    def _():
        for m in range(1, nc):
            a_copy(m).wait_send()

    for k in range(1, nd):
        rs_copy(k).wait_send()
        ag_copy(k).wait_send()

    @pl.loop(0, nd)
    def _(b):
        for ch in range(chunks):
            @pl.when(b > z)
            def _():
                up_copy(b, ch).wait_send()

            @pl.when(b < z)
            def _():
                down_copy(b, ch).wait_send()


def local(sizes, a_tile, panels):
    nr, nc, nd = sizes
    tile_rows, tile_cols = a_tile.shape
    k_size = panels.shape[1]
    share, crows = tile_rows // nd, tile_rows // nc
    piece, chunks, slab = crows // nd, tile_cols // CHUNK, PB // nc
    high = max(8, slab // nd)
    split_d = (high, slab * PB // (nd * high))
    vmem = pl.BlockSpec(memory_space=pltpu.VMEM)
    shape = lambda *s: jax.ShapeDtypeStruct(s, F32)
    dma = lambda *s: pltpu.SemaphoreType.DMA(s)
    wide = max(PB, tile_cols)
    trailing, new_panel, norm = pl.pallas_call(
        functools.partial(gather_update, sizes, split_d),
        out_shape=(shape(share, tile_cols), shape(crows, PB), shape(1, 1)),
        in_specs=[vmem] * 2,
        out_specs=(vmem,) * 3,
        scratch_shapes=[
            pltpu.VMEM((tile_rows, k_size), BF16), pltpu.VMEM((tile_rows, k_size), BF16),
            pltpu.VMEM((wide, k_size), BF16), pltpu.VMEM((wide, k_size), BF16),
            pltpu.VMEM((PB, k_size), F32), pltpu.VMEM((tile_cols, k_size), F32),
            pltpu.VMEM((tile_rows, tile_cols), F32), pltpu.VMEM((tile_rows, tile_cols), F32),
            pltpu.VMEM((tile_rows, tile_cols), F32), pltpu.VMEM((crows, PB), F32),
            pltpu.VMEM((nd, piece, PB), F32), pltpu.VMEM((piece, PB), F32),
            pltpu.VMEM((nr + nc + nd, 8, CHUNK), F32), pltpu.VMEM((4, 8, CHUNK), F32),
            dma(2), dma(2), dma(nc), pltpu.SemaphoreType.DMA, dma(nd), dma(nd), dma(nd), dma(nd),
            dma(nd, nc), dma(nd, nc), dma(nd, nc), dma(nd, nc),
            dma(nd, chunks), dma(nd, chunks), dma(nd, chunks), dma(nd, chunks),
            dma(nr + nc + nd), dma(nr + nc + nd),
            pltpu.VMEM((crows, PB), F32), pltpu.VMEM((PB, PB), F32), pltpu.VMEM((BLOCK, 2 * BLOCK), F32),
            pltpu.VMEM((PB // BLOCK, BLOCK, BLOCK), F32), pltpu.VMEM((PB, PB), F32), pltpu.VMEM((crows, PB), F32),
            pltpu.VMEM((slab, PB), F32), pltpu.VMEM((nd, *split_d), F32), pltpu.VMEM(split_d, F32),
            dma(nd), dma(nd), dma(nd), dma(nd), dma(nc), pltpu.SemaphoreType.DMA,
        ],
        compiler_params=pltpu.CompilerParams(collective_id=0, has_side_effects=True, vmem_limit_bytes=60 << 20),
        name="gather_update",
    )(a_tile, panels)
    return (trailing, new_panel, norm.reshape(1))


def solution(mesh):
    sizes = tuple(mesh.shape[axis] for axis in ("row", "col", "depth"))
    return jax.shard_map(
        functools.partial(local, sizes),
        mesh=mesh,
        in_specs=(P("row", "col"), P("row", "depth")),
        out_specs=(P(("row", "depth"), "col"), P(("row", "col"), None), P()),
        check_vma=False,
    )
```
